512 devices in a mesh: segment: 16 (over x_hi, y, core), row: 32 (over x_lo, z).
Axes of the slice: x: 4 (x_hi: 2, x_lo: 2; x = x_hi * 2 + x_lo), y: 4, z: 16, core: 2. Of those that a mesh axis runs over, the one named last changes fastest.
Arguments:
- image_slabs: float32 [2, 64, 64, 128], P(None, 'row'), may hold values from -6 to 6
- first_kernel: float32 [16, 3, 3, 128, 128], P('segment'), may hold values from -0.1875 to 0.1875
- second_kernel: float32 [16, 3, 3, 128, 128], P('segment'), may hold values from -0.1875 to 0.1875
- skip_kernel: float32 [8, 128, 128], replicated, may hold values from -0.5 to 0.5
- first_gain: float32 [16, 128], P('segment'), may hold values from 0.5 to 2
- first_bias: float32 [16, 128], P('segment'), may hold values from -1.5 to 1.5
- second_gain: float32 [16, 128], P('segment'), may hold values from 0.5 to 2
- second_bias: float32 [16, 128], P('segment'), may hold values from -1.5 to 1.5
Outputs:
- level_out: float32 [2, 64, 64, 128], P(None, 'row', 'segment')
The draws below stay inside these ranges and needn't reach their ends.
All inputs are finite; a program needn't handle non-finite values.
Results may differ from the reference program's by a relative error of at most 0.00018.
Values sent between devices are 32-bit elements; how exact they have to be, the bound alone decides.
A program may use at most 64 MiB of HBM per device.

```python
import math
import jax
import jax.numpy as jnp
from jax import lax

C = 128
WIDTH = 64
MICRO = 2
SECTIONS = 16
HALF = 8
ROWS = 64
N_SEGMENT = 16


def block_scale(stream_key, dims, shards, low, largest):
    loudness = 1.0
    for dim, shards_of in shards:
        heights = jax.random.uniform(jax.random.fold_in(jax.random.fold_in(stream_key, 6), dim), (shards_of,), jnp.float32, low / len(shards), largest / len(shards))
        loudness = loudness * jnp.repeat(jnp.exp(heights), dims[dim] // shards_of).reshape((-1,) + (1,) * (len(dims) - 1 - dim))
    return loudness


def normal_values(key, shape, spread, limit, cuts=(), kind=jnp.bfloat16):
    gain = block_scale(key, shape, cuts, -0.22, 0.18) if cuts else 1.0
    drawn = jax.random.normal(key, shape, jnp.float32) * spread * gain
    return jnp.minimum(jnp.maximum(drawn, -limit), limit).astype(kind)


def setup_inputs(seed: int = 0) -> dict:
    key_list = jax.random.split(jax.random.key(seed), 9)
    return {
        "image_slabs": normal_values(key_list[0], (MICRO, ROWS, WIDTH, C), 1.0, 6.0, ((1, 32),), jnp.float32),
        "first_kernel": normal_values(key_list[1], (SECTIONS, 3, 3, C, C), (9 * C) ** -0.5, 0.1875, ((0, 16),), jnp.float32),
        "second_kernel": normal_values(key_list[2], (SECTIONS, 3, 3, C, C), (9 * C) ** -0.5, 0.1875, ((0, 16),), jnp.float32),
        "skip_kernel": normal_values(key_list[3], (HALF, C, C), C ** -0.5, 0.5, (), jnp.float32),
        "first_gain": jnp.clip(jnp.exp(math.log(2.0) - 1.3862944 * jax.random.uniform(key_list[4], (SECTIONS, C), jnp.float32) ** block_scale(key_list[4], (SECTIONS, C), ((0, 16),), -0.2, 0.2)), 0.5, 2.0),
        "first_bias": normal_values(key_list[5], (SECTIONS, C), 0.3, 1.5, ((0, 16),), jnp.float32),
        "second_gain": jnp.clip(jnp.exp(math.log(2.0) - 1.3862944 * jax.random.uniform(key_list[6], (SECTIONS, C), jnp.float32) ** block_scale(key_list[6], (SECTIONS, C), ((0, 16),), -0.2, 0.2)), 0.5, 2.0),
        "second_bias": normal_values(key_list[7], (SECTIONS, C), 0.3, 1.5, ((0, 16),), jnp.float32),
    }


def convolve(current, kernel):
    height, breadth, channels = current.shape
    padded = jnp.pad(current, ((1, 1), (1, 1), (0, 0)))
    summed = jnp.zeros((height * breadth, kernel.shape[3]), jnp.float32)
    for row_step in range(3):
        for col_step in range(3):
            window = padded[row_step:row_step + height, col_step:col_step + breadth].reshape(height * breadth, channels)
            summed = summed + jnp.dot(window, kernel[row_step, col_step], precision=lax.Precision.HIGHEST, preferred_element_type=jnp.float32)
    return summed.reshape(height, breadth, kernel.shape[3])


def section(current, kernel_one, kernel_two, gain_one, bias_one, gain_two, bias_two, skip_term):
    hidden = jax.nn.silu(gain_one * convolve(current, kernel_one) + bias_one)
    return current + jax.nn.silu(gain_two * (convolve(hidden, kernel_two) + skip_term) + bias_two)


def reference(image_slabs, first_kernel, second_kernel, skip_kernel, first_gain, first_bias, second_gain, second_bias):
    half_count = N_SEGMENT // 2
    outputs = []
    for micro_index in range(image_slabs.shape[0]):
        current = image_slabs[micro_index]
        encoder_outs = []
        for section_index in range(N_SEGMENT):
            if section_index < half_count:
                skip_term = jnp.zeros_like(current)
            else:
                source = encoder_outs[2 * half_count - 1 - section_index]
                channels = current.shape[2]
                skip_term = jnp.dot(source.reshape(-1, channels), skip_kernel[section_index - half_count], precision=lax.Precision.HIGHEST, preferred_element_type=jnp.float32).reshape(current.shape)
            current = section(current, first_kernel[section_index], second_kernel[section_index], first_gain[section_index], first_bias[section_index], second_gain[section_index], second_bias[section_index], skip_term)
            if section_index < half_count:
                encoder_outs.append(current)
        outputs.append(current)
    return jnp.stack(outputs)
```

```python
import functools

import jax
import jax.numpy as jnp
from jax import lax
from jax.experimental import pallas as pl
from jax.experimental.pallas import tpu as pltpu
from jax.sharding import PartitionSpec as P

MESH = pl.DeviceIdType.MESH
C = 128
TILE = 32
RING = 40
STRIP = 8


def split(x):
    high = x.astype(jnp.bfloat16).astype(jnp.float32)
    return high, x - high


def silu(u):
    return u / (1.0 + jnp.exp(-u))


def level_kernel(
    n_seg,
    n_row,
    img,
    w1,
    w2,
    skipk,
    g1,
    b1,
    g2,
    b2,
    out,
    xbuf,
    xh,
    xl,
    hh,
    hl,
    h1,
    yout,
    fin,
    landed,
    pw1,
    pw2,
    pvec,
    vecs,
    wp,
    ska,
    skb,
    ea,
    eb,
    m0,
    m2,
    wsend,
    wrecv,
    gsend,
    grecv,
    msend,
    mrecv,
    ssend,
    srecv,
    fsend,
    frecv,
):
    stages = n_seg // 2
    mirror = stages // 2
    groups = n_row // 2
    pieces = n_seg // 2
    cw = 2 * TILE // n_seg
    s = lax.axis_index("segment")
    r = lax.axis_index("row")
    m = s // 2
    c = s % 2
    g = r // 2
    half = r % 2
    up = (g > 0).astype(jnp.int32)
    down = (g < groups - 1).astype(jnp.int32)
    valid = 1 + up + down
    inside = {-1: g > 0, 0: g >= 0, 1: g < groups - 1}

    def greet(cond, seg, row):
        @pl.when(cond)
        def _():
            pl.semaphore_signal(barrier, inc=1, device_id=(seg, row), device_id_type=MESH)

    xbuf[...] = jnp.zeros_like(xbuf)

    barrier = pltpu.get_barrier_semaphore()
    greet(s >= 0, s + 1 - 2 * c, r)
    for d in (-1, 0, 1):
        greet(inside[d] & (m > 0), s - 2, r + 2 * d)
        greet(inside[d] & (m > 0), s - 2, r + 1 - 2 * half + 2 * d)
        for q in (0, 1):
            other = 2 * (g + d) + q
            greet(inside[d] & (m == 0) & (other != r), s, other)
    greet(m > mirror, 2 * (stages - m) + c, r)
    greet(m >= mirror, 2 * (stages - 1 - m) + c, r)
    source = 2 * g + s // pieces
    for k in (0, 1):
        last = n_seg - 2 + k
        greet((s != last) | (r != source), last, source)

    one = jnp.int32(1)
    zero = jnp.int32(0)
    expected = (
        1
        + jnp.where(m < stages - 1, 2 * valid, zero)
        + jnp.where(m == 0, 2 * valid - 1, zero)
        + jnp.where((m > 0) & (m < mirror), one, zero)
        + jnp.where(m < mirror, one, zero)
        + jnp.where(m == stages - 1, 2 * pieces - half, zero)
    )
    pl.semaphore_wait(barrier, expected)

    def swaps():
        pairs = [(w1, pw1), (w2, pw2)] + [(v, pvec.at[i]) for i, v in enumerate((g1, b1, g2, b2))]
        return [
            pltpu.make_async_remote_copy(
                src_ref=a,
                dst_ref=b,
                send_sem=wsend.at[i],
                recv_sem=wrecv.at[i],
                device_id=(s + 1 - 2 * c, r),
                device_id_type=MESH,
            )
            for i, (a, b) in enumerate(pairs)
        ]

    swap = swaps()

    def gathers(start):
        for d in (-1, 0, 1):
            for q in (0, 1):
                other = 2 * (g + d) + q
                offset = 2 * half - 4 * d + 4
                index = (2 * (1 - d) + half) * 2
                strip = TILE if q == 0 else TILE - STRIP

                @pl.when((m == 0) & inside[d] & (other != r))
                def _():
                    for kind, (a, b) in enumerate(
                        (
                            (img.at[c, :, TILE * q : TILE * q + TILE, :], (0, TILE)),
                            (img.at[c, :, strip : strip + STRIP, :], (TILE, STRIP)),
                        )
                    ):
                        copy = pltpu.make_async_remote_copy(
                            src_ref=a,
                            dst_ref=xbuf.at[pl.ds(offset, 2), b[0] : b[0] + b[1], :],
                            send_sem=gsend.at[((d + 1) * 2 + q) * 2 + kind],
                            recv_sem=grecv.at[index + kind],
                            device_id=(s, other),
                            device_id_type=MESH,
                        )
                        if start:
                            copy.start()
                        else:
                            copy.wait_send()

    gathers(True)
    for copy in swap:
        copy.start()

    column = lax.broadcasted_iota(jnp.int32, (RING, C), 0)
    m0[...] = jnp.where((column == 0) & (half == 0), 0.0, 1.0)
    m2[...] = jnp.where((column == TILE - 1) & (half == 1), 0.0, 1.0)

    def prepare(slot, conv, ref):
        for a in range(3):
            for b in range(3):
                high, low = split(ref[0, a, b])
                cols = pl.ds(b * C, C)
                wp[slot, conv, pl.ds(a * C, C), cols] = high
                wp[slot, conv, pl.ds((3 + a) * C, C), cols] = high
                wp[slot, conv, pl.ds((6 + a) * C, C), cols] = low

    prepare(c, 0, w1)
    prepare(c, 1, w2)
    for i, v in enumerate((g1, b1, g2, b2)):
        vecs[c, i] = v[...]
    swap[0].wait_recv()
    prepare(1 - c, 0, pw1)
    swap[1].wait_recv()
    prepare(1 - c, 1, pw2)
    for i in range(4):
        swap[2 + i].wait_recv()
        vecs[1 - c, i] = pvec[i]

    def skip_term(src, dst, which):
        rows = src.shape[0]
        xv, xw = split(src[...].reshape(rows * RING, C))
        kh, kl = split(skipk[which])
        dot = functools.partial(jnp.dot, preferred_element_type=jnp.float32)
        term = dot(xv, kh) + (dot(xv, kl) + dot(xw, kh))
        dst[...] = term.reshape(rows, RING, C)

    ea[...] = jnp.zeros_like(ea)
    eb[...] = jnp.zeros_like(eb)

    def forward_a():
        return pltpu.make_async_remote_copy(
            src_ref=xbuf.at[2:10],
            dst_ref=ska,
            send_sem=ssend.at[0],
            recv_sem=srecv.at[0],
            device_id=(2 * (stages - m) + c, r),
            device_id_type=MESH,
        )

    def forward_b():
        return pltpu.make_async_remote_copy(
            src_ref=h1.at[4:8],
            dst_ref=skb,
            send_sem=ssend.at[1],
            recv_sem=srecv.at[1],
            device_id=(2 * (stages - 1 - m) + c, r),
            device_id_type=MESH,
        )

    @pl.when(m > mirror)
    def _():
        forward_a().wait_recv()
        skip_term(ska, ea, jnp.maximum(2 * (m - mirror), 0))

    @pl.when(m >= mirror)
    def _():
        forward_b().wait_recv()
        skip_term(skb, eb, jnp.maximum(2 * (m - mirror) + 1, 0))

    def handover(d, kind):
        slot = 1 - d
        if kind == 0:
            src = yout
            dst = xbuf.at[4 * slot : 4 * slot + 4, 0:TILE, :]
            row = r + 2 * d
        else:
            src = yout.at[:, pl.ds(pl.multiple_of((TILE - STRIP) * (1 - half), STRIP), STRIP), :]
            dst = xbuf.at[4 * slot : 4 * slot + 4, TILE:RING, :]
            row = r + 1 - 2 * half + 2 * d
        return pltpu.make_async_remote_copy(
            src_ref=src,
            dst_ref=dst,
            send_sem=msend.at[2 * (d + 1) + kind],
            recv_sem=mrecv.at[2 * slot + kind],
            device_id=(s + 2, row),
            device_id_type=MESH,
        )

    for d in (-1, 0, 1):

        @pl.when((m == 0) & inside[d])
        def _():
            for p in (0, 1):
                index = (2 * (1 + d) + p) * 2

                @pl.when((2 * (g + d) + p) != r)
                def _():
                    for kind, b in enumerate(((0, TILE), (TILE, STRIP))):
                        rows = 2 * p + 4 * d + 4
                        pltpu.make_async_remote_copy(
                            src_ref=xbuf.at[rows : rows + 2, b[0] : b[0] + b[1], :],
                            dst_ref=xbuf.at[rows : rows + 2, b[0] : b[0] + b[1], :],
                            send_sem=gsend.at[0],
                            recv_sem=grecv.at[index + kind],
                            device_id=(s, r),
                            device_id_type=MESH,
                        ).wait_recv()

        @pl.when((m > 0) & inside[d])
        def _():
            for kind in (0, 1):
                handover(-d, kind).wait_recv()

    for q in (0, 1):

        @pl.when((m == 0) & (half == q))
        def _():
            strip = TILE if q == 0 else TILE - STRIP
            xbuf[4 + 2 * q : 6 + 2 * q, 0:TILE, :] = img[c, :, TILE * q : TILE * q + TILE, :]
            xbuf[4 + 2 * q : 6 + 2 * q, TILE:RING, :] = img[c, :, strip : strip + STRIP, :]

    @pl.when((m > 0) & (m < mirror))
    def _():
        forward_a().start()

    @pl.when(m == mirror)
    def _():
        skip_term(xbuf.at[2:10], ea, 0)

    def conv(high, low, first, rows, slot, which):
        def part(ref, a):
            return ref[first - 1 + a : first - 1 + a + rows].reshape(rows * RING, C)

        hs = [part(high, a) for a in range(3)]
        ls = [part(low, a) for a in range(3)]
        left = jnp.concatenate(hs + ls + hs, axis=1)
        acc = jnp.dot(left, wp[slot, which], preferred_element_type=jnp.float32)
        left_tap, middle, right_tap = [
            acc[:, b * C : (b + 1) * C].reshape(rows, RING, C) for b in range(3)
        ]
        return (
            pltpu.roll(left_tap, 1, 1) * m0[...][None]
            + middle
            + pltpu.roll(right_tap, RING - 1, 1) * m2[...][None]
        )

    def inside_rows(value, first):
        row = 4 * g - 4 + first + lax.broadcasted_iota(jnp.int32, value.shape, 0)
        return jnp.where((row >= 0) & (row < 4 * groups), value, 0.0)

    def vec(slot, i):
        return vecs[slot, i].reshape(1, 1, C)

    def store_split(high, low, first, value):
        top, rest = split(value)
        high[first : first + value.shape[0]] = top
        low[first : first + value.shape[0]] = rest

    store_split(xh, xl, 0, xbuf[...])
    hidden = inside_rows(silu(vec(0, 0) * conv(xh, xl, 1, 10, 0, 0) + vec(0, 1)), 1)
    store_split(hh, hl, 1, hidden)
    value = xbuf[2:10] + silu(vec(0, 2) * (conv(hh, hl, 2, 8, 0, 1) + ea[...]) + vec(0, 3))
    value = inside_rows(value, 2)
    h1[2:10] = value
    store_split(xh, xl, 2, value)

    @pl.when(m < mirror)
    def _():
        forward_b().start()

    hidden = inside_rows(silu(vec(1, 0) * conv(xh, xl, 3, 6, 1, 0) + vec(1, 1)), 3)
    store_split(hh, hl, 3, hidden)
    value = h1[4:8] + silu(vec(1, 2) * (conv(hh, hl, 4, 4, 1, 1) + eb[...]) + vec(1, 3))
    value = value[:, 0:TILE]

    @pl.when(m < stages - 1)
    def _():
        yout[...] = value
        for kind in (0, 1):
            for d in (-1, 1, 0):

                @pl.when(inside[d])
                def _():
                    handover(d, kind).start()

    def scatter(i, p):
        return pltpu.make_async_remote_copy(
            src_ref=fin.at[i, 2 * p : 2 * p + 2],
            dst_ref=landed.at[c],
            send_sem=fsend.at[2 * i + p],
            recv_sem=frecv.at[c],
            device_id=(pieces * half + i, 2 * g + p),
            device_id_type=MESH,
        )

    def each_piece(action):
        for i in range(pieces):
            for p in (0, 1):

                @pl.when((pieces * half + i != s) | (2 * g + p != r))
                def _():
                    action(scatter(i, p))

    @pl.when(m == stages - 1)
    def _():
        for i in range(pieces):
            fin[i] = value[:, i * cw : (i + 1) * cw, :]
        each_piece(lambda copy: copy.start())

        @pl.when(half == 1)
        def _():
            landed[c] = fin[pieces - 2 + c, 2:4]

    for k in (0, 1):

        @pl.when((s != n_seg - 2 + k) | (r != source))
        def _():
            pltpu.make_async_remote_copy(
                src_ref=fin.at[0, 0:2],
                dst_ref=landed.at[k],
                send_sem=fsend.at[0],
                recv_sem=frecv.at[k],
                device_id=(s, r),
                device_id_type=MESH,
            ).wait_recv()

    out[...] = landed[...]

    for copy in swap:
        copy.wait_send()
    gathers(False)

    @pl.when(m < stages - 1)
    def _():
        for kind in (0, 1):
            for d in (-1, 0, 1):

                @pl.when(inside[d])
                def _():
                    handover(d, kind).wait_send()

    @pl.when((m > 0) & (m < mirror))
    def _():
        forward_a().wait_send()

    @pl.when(m < mirror)
    def _():
        forward_b().wait_send()

    @pl.when(m == stages - 1)
    def _():
        each_piece(lambda copy: copy.wait_send())


def solution(mesh):
    n_seg = mesh.shape["segment"]
    n_row = mesh.shape["row"]
    pieces = n_seg // 2
    cw = 2 * TILE // n_seg
    f32 = jnp.float32
    vmem = pl.BlockSpec(memory_space=pltpu.VMEM)

    def on_device(*args):
        dma = pltpu.SemaphoreType.DMA
        return pl.pallas_call(
            functools.partial(level_kernel, n_seg, n_row),
            out_shape=jax.ShapeDtypeStruct((2, 2, cw, C), f32),
            in_specs=[vmem] * 8,
            out_specs=vmem,
            scratch_shapes=[
                pltpu.VMEM((12, RING, C), f32),
                pltpu.VMEM((12, RING, C), f32),
                pltpu.VMEM((12, RING, C), f32),
                pltpu.VMEM((12, RING, C), f32),
                pltpu.VMEM((12, RING, C), f32),
                pltpu.VMEM((12, RING, C), f32),
                pltpu.VMEM((4, TILE, C), f32),
                pltpu.VMEM((pieces, 4, cw, C), f32),
                pltpu.VMEM((2, 2, cw, C), f32),
                pltpu.VMEM((1, 3, 3, C, C), f32),
                pltpu.VMEM((1, 3, 3, C, C), f32),
                pltpu.VMEM((4, 1, C), f32),
                pltpu.VMEM((2, 4, 1, C), f32),
                pltpu.VMEM((2, 2, 9 * C, 3 * C), f32),
                pltpu.VMEM((8, RING, C), f32),
                pltpu.VMEM((4, RING, C), f32),
                pltpu.VMEM((8, RING, C), f32),
                pltpu.VMEM((4, RING, C), f32),
                pltpu.VMEM((RING, C), f32),
                pltpu.VMEM((RING, C), f32),
                dma((6,)),
                dma((6,)),
                dma((12,)),
                dma((12,)),
                dma((6,)),
                dma((6,)),
                dma((2,)),
                dma((2,)),
                dma((2 * pieces,)),
                dma((2,)),
            ],
            compiler_params=pltpu.CompilerParams(
                collective_id=0, has_side_effects=True, vmem_limit_bytes=48 * 1024 * 1024
            ),
        )(*args)

    return jax.shard_map(
        on_device,
        mesh=mesh,
        in_specs=(
            P(None, "row", None, None),
            P("segment", None, None, None, None),
            P("segment", None, None, None, None),
            P(),
            P("segment", None),
            P("segment", None),
            P("segment", None),
            P("segment", None),
        ),
        out_specs=P(None, "row", "segment", None),
        check_vma=False,
    )
```

```python
import functools

import jax
import jax.numpy as jnp
from jax import lax
from jax.experimental import pallas as pl
from jax.experimental.pallas import tpu as pltpu
from jax.sharding import PartitionSpec as P

MESH = pl.DeviceIdType.MESH
C = 128
TILE = 32
RING = 40
STRIP = 8


def split(x):
    high = x.astype(jnp.bfloat16).astype(jnp.float32)
    return high, x - high


def silu(u):
    return u / (1.0 + jnp.exp(-u))


def level_kernel(
    n_seg,
    n_row,
    img_hbm,
    w1_hbm,
    w2_hbm,
    skipk_hbm,
    g1_hbm,
    b1_hbm,
    g2_hbm,
    b2_hbm,
    out,
    img,
    w1,
    w2,
    skipk,
    ovec,
    sout,
    sin,
    xbuf,
    xh,
    xl,
    hh,
    hl,
    h1,
    yout,
    fin,
    landed,
    pw1,
    pw2,
    pvec,
    vecs,
    wp,
    ska,
    skb,
    ea,
    eb,
    m0,
    m2,
    wsend,
    wrecv,
    gsend,
    grecv,
    msend,
    mrecv,
    ssend,
    srecv,
    fsend,
    frecv,
    lsem,
):
    stages = n_seg // 2
    mirror = stages // 2
    groups = n_row // 2
    pieces = n_seg // 2
    cw = 2 * TILE // n_seg
    s = lax.axis_index("segment")
    r = lax.axis_index("row")
    m = s // 2
    c = s % 2
    g = r // 2
    slab = r % 2
    up = (g > 0).astype(jnp.int32)
    down = (g < groups - 1).astype(jnp.int32)
    valid = 1 + up + down
    inside = {-1: g > 0, 0: g >= 0, 1: g < groups - 1}

    def greet(cond, seg, row):
        @pl.when(cond)
        def _():
            pl.semaphore_signal(barrier, inc=1, device_id=(seg, row), device_id_type=MESH)

    first_skip = jnp.maximum(2 * (m - mirror), 0)
    loads = [
        pltpu.make_async_copy(a, b, lsem.at[i])
        for i, (a, b) in enumerate(
            [
                (img_hbm, img),
                (w1_hbm, w1),
                (w2_hbm, w2),
                (skipk_hbm.at[pl.ds(first_skip, 2)], skipk),
                (g1_hbm, ovec.at[0]),
                (b1_hbm, ovec.at[1]),
                (g2_hbm, ovec.at[2]),
                (b2_hbm, ovec.at[3]),
            ]
        )
    ]
    for copy in loads:
        copy.start()

    xbuf[...] = jnp.zeros_like(xbuf)
    sin[...] = jnp.zeros_like(sin)

    barrier = pltpu.get_barrier_semaphore()
    greet(s >= 0, s + 1 - 2 * c, r)
    for d in (-1, 0, 1):
        greet(inside[d] & (m > 0), s - 2, r + 2 * d)
        greet(inside[d] & (m > 0), s - 1 - 2 * c, r + 2 * d)
        for q in (0, 1):
            other = 2 * (g + d) + q
            greet(inside[d] & (m == 0) & (other != r), s, other)
    greet(m > mirror, 2 * (stages - m) + c, r)
    greet(m >= mirror, 2 * (stages - 1 - m) + c, r)
    source = n_seg - 2 + s // pieces
    for k in (0, 1):
        greet((s != source) | (r != 2 * g + k), source, 2 * g + k)

    one = jnp.int32(1)
    zero = jnp.int32(0)
    expected = (
        1
        + jnp.where(m < stages - 1, 2 * valid, zero)
        + jnp.where(m == 0, 2 * valid - 1, zero)
        + jnp.where((m > 0) & (m < mirror), one, zero)
        + jnp.where(m < mirror, one, zero)
        + jnp.where(m == stages - 1, 2 * pieces - c, zero)
    )
    pl.semaphore_wait(barrier, expected)

    def swaps():
        pairs = [(w1, pw1), (w2, pw2), (ovec, pvec)]
        return [
            pltpu.make_async_remote_copy(
                src_ref=a,
                dst_ref=b,
                send_sem=wsend.at[i],
                recv_sem=wrecv.at[i],
                device_id=(s + 1 - 2 * c, r),
                device_id_type=MESH,
            )
            for i, (a, b) in enumerate(pairs)
        ]

    swap = swaps()

    own = pl.ds(pl.multiple_of(TILE * c, TILE), TILE)
    strip = pl.ds(pl.multiple_of(TILE - STRIP * c, STRIP), STRIP)

    def gathers(start):
        for d in (-1, 1, 0):
            for q in (0, 1):
                other = 2 * (g + d) + q
                offset = 2 * slab - 4 * d + 4
                index = (2 * (1 - d) + slab) * 2

                @pl.when((m == 0) & inside[d] & (other != r))
                def _():
                    for kind, (a, b) in enumerate(
                        (
                            (img.at[q, :, own, :], (0, TILE)),
                            (img.at[q, :, strip, :], (TILE, STRIP)),
                        )
                    ):
                        copy = pltpu.make_async_remote_copy(
                            src_ref=a,
                            dst_ref=xbuf.at[pl.ds(offset, 2), b[0] : b[0] + b[1], :],
                            send_sem=gsend.at[((d + 1) * 2 + q) * 2 + kind],
                            recv_sem=grecv.at[index + kind],
                            device_id=(s, other),
                            device_id_type=MESH,
                        )
                        if start:
                            copy.start()
                        else:
                            copy.wait_send()

    loads[0].wait()
    gathers(True)

    for copy in loads[1:]:
        copy.wait()
    for copy in swap:
        copy.start()

    column = lax.broadcasted_iota(jnp.int32, (RING, C), 0)
    m0[...] = jnp.where((column == 0) & (c == 0), 0.0, 1.0)
    m2[...] = jnp.where((column == TILE - 1) & (c == 1), 0.0, 1.0)

    def prepare(slot, conv, ref):
        for a in range(3):
            for b in range(3):
                high, low = split(ref[0, a, b])
                cols = pl.ds(b * C, C)
                wp[slot, conv, pl.ds(a * C, C), cols] = high
                wp[slot, conv, pl.ds((3 + a) * C, C), cols] = high
                wp[slot, conv, pl.ds((6 + a) * C, C), cols] = low

    prepare(c, 0, w1)
    prepare(c, 1, w2)
    vecs[c] = ovec[...]
    swap[0].wait_recv()
    prepare(1 - c, 0, pw1)
    swap[1].wait_recv()
    prepare(1 - c, 1, pw2)
    swap[2].wait_recv()
    vecs[1 - c] = pvec[...]

    def skip_term(src, dst, which):
        rows, columns = src.shape[:2]
        xv, xw = split(src[...].reshape(rows * columns, C))
        kh, kl = split(skipk[which])
        dot = functools.partial(jnp.dot, preferred_element_type=jnp.float32)
        term = dot(xv, kh) + (dot(xv, kl) + dot(xw, kh))
        dst[...] = term.reshape(rows, columns, C)

    ea[...] = jnp.zeros_like(ea)
    eb[...] = jnp.zeros_like(eb)

    def forward_a():
        return pltpu.make_async_remote_copy(
            src_ref=xbuf.at[2:10],
            dst_ref=ska,
            send_sem=ssend.at[0],
            recv_sem=srecv.at[0],
            device_id=(2 * (stages - m) + c, r),
            device_id_type=MESH,
        )

    def forward_b():
        return pltpu.make_async_remote_copy(
            src_ref=h1.at[4:8, 0:TILE],
            dst_ref=skb,
            send_sem=ssend.at[1],
            recv_sem=srecv.at[1],
            device_id=(2 * (stages - 1 - m) + c, r),
            device_id_type=MESH,
        )

    @pl.when(m > mirror)
    def _():
        forward_a().wait_recv()
        skip_term(ska, ea, 0)

    def second_skip():
        forward_b().wait_recv()
        skip_term(skb, eb, 1)

    @pl.when(m > mirror)
    def _():
        second_skip()

    def handover(d, kind):
        slot = 1 - d
        if kind == 0:
            src = yout
            dst = xbuf.at[4 * slot : 4 * slot + 4, 0:TILE, :]
            seg = s + 2
        else:
            src = sout
            dst = sin.at[4 * slot : 4 * slot + 4]
            seg = s + 3 - 2 * c
        return pltpu.make_async_remote_copy(
            src_ref=src,
            dst_ref=dst,
            send_sem=msend.at[2 * (d + 1) + kind],
            recv_sem=mrecv.at[2 * slot + kind],
            device_id=(seg, r + 2 * d),
            device_id_type=MESH,
        )

    for d in (-1, 0, 1):

        @pl.when((m == 0) & inside[d])
        def _():
            for p in (0, 1):
                index = (2 * (1 + d) + p) * 2

                @pl.when((2 * (g + d) + p) != r)
                def _():
                    for kind, b in enumerate(((0, TILE), (TILE, STRIP))):
                        rows = 2 * p + 4 * d + 4
                        pltpu.make_async_remote_copy(
                            src_ref=xbuf.at[rows : rows + 2, b[0] : b[0] + b[1], :],
                            dst_ref=xbuf.at[rows : rows + 2, b[0] : b[0] + b[1], :],
                            send_sem=gsend.at[0],
                            recv_sem=grecv.at[index + kind],
                            device_id=(s, r),
                            device_id_type=MESH,
                        ).wait_recv()

        @pl.when((m > 0) & inside[d])
        def _():
            for kind in (0, 1):
                handover(-d, kind).wait_recv()

    for q in (0, 1):

        @pl.when((m == 0) & (slab == q))
        def _():
            xbuf[4 + 2 * q : 6 + 2 * q, 0:TILE, :] = img[q, :, own, :]
            xbuf[4 + 2 * q : 6 + 2 * q, TILE:RING, :] = img[q, :, strip, :]

    @pl.when(m > 0)
    def _():
        xbuf[:, TILE : TILE + 4] = sin[...]
        xbuf[:, TILE + 4 : RING] = sin[...]

    @pl.when(m == mirror)
    def _():
        skip_term(xbuf.at[2:10], ea, 0)
        second_skip()

    def conv(high, low, first, rows, slot, which):
        def part(ref, a):
            return ref[first - 1 + a : first - 1 + a + rows].reshape(rows * RING, C)

        hs = [part(high, a) for a in range(3)]
        ls = [part(low, a) for a in range(3)]
        left = jnp.concatenate(hs + ls + hs, axis=1)
        acc = jnp.dot(left, wp[slot, which], preferred_element_type=jnp.float32)
        left_tap, middle, right_tap = [
            acc[:, b * C : (b + 1) * C].reshape(rows, RING, C) for b in range(3)
        ]
        return (
            pltpu.roll(left_tap, 1, 1) * m0[...][None]
            + middle
            + pltpu.roll(right_tap, RING - 1, 1) * m2[...][None]
        )

    def inside_rows(value, first):
        row = 4 * g - 4 + first + lax.broadcasted_iota(jnp.int32, value.shape, 0)
        return jnp.where((row >= 0) & (row < 4 * groups), value, 0.0)

    def vec(slot, i):
        return vecs[slot, i].reshape(1, 1, C)

    def store_split(high, low, first, value):
        top, rest = split(value)
        high[first : first + value.shape[0]] = top
        low[first : first + value.shape[0]] = rest

    store_split(xh, xl, 0, xbuf[...])
    hidden = inside_rows(silu(vec(0, 0) * conv(xh, xl, 1, 10, 0, 0) + vec(0, 1)), 1)
    store_split(hh, hl, 1, hidden)
    value = xbuf[2:10] + silu(vec(0, 2) * (conv(hh, hl, 2, 8, 0, 1) + ea[...]) + vec(0, 3))
    value = inside_rows(value, 2)
    h1[2:10] = value
    store_split(xh, xl, 2, value)

    @pl.when(m == mirror - 1)
    def _():
        forward_b().start()

    hidden = inside_rows(silu(vec(1, 0) * conv(xh, xl, 3, 6, 1, 0) + vec(1, 1)), 3)
    store_split(hh, hl, 3, hidden)
    second = conv(hh, hl, 4, 4, 1, 1)[:, 0:TILE] + eb[...]
    value = h1[4:8, 0:TILE] + silu(vec(1, 2) * second + vec(1, 3))

    def handovers(action):
        for d, kind in ((-1, 1), (1, 1), (-1, 0), (1, 0), (0, 1), (0, 0)):

            @pl.when(inside[d])
            def _():
                action(handover(d, kind))

    @pl.when(m < stages - 1)
    def _():
        yout[...] = value
        sout[...] = jnp.where(c == 0, value[:, TILE - 4 :], value[:, :4])
        handovers(lambda copy: copy.start())
        handovers(lambda copy: copy.wait_send())

    @pl.when((m > 0) & (m < mirror))
    def _():
        forward_a().start()

    @pl.when(m < mirror - 1)
    def _():
        forward_b().start()

    def scatter(i, p):
        return pltpu.make_async_remote_copy(
            src_ref=fin.at[i, 2 * p : 2 * p + 2],
            dst_ref=landed.at[slab],
            send_sem=fsend.at[2 * i + p],
            recv_sem=frecv.at[slab],
            device_id=(pieces * c + i, 2 * g + p),
            device_id_type=MESH,
        )

    def each_piece(action):
        for i in range(pieces):
            for p in (0, 1):

                @pl.when((pieces * c + i != s) | (2 * g + p != r))
                def _():
                    action(scatter(i, p))

    @pl.when(m == stages - 1)
    def _():
        for i in range(pieces):
            fin[i] = value[:, i * cw : (i + 1) * cw, :]
        each_piece(lambda copy: copy.start())

        for p in (0, 1):

            @pl.when((c == 1) & (slab == p))
            def _():
                landed[p] = fin[pieces - 1, 2 * p : 2 * p + 2]

    for k in (0, 1):

        @pl.when((s != source) | (r != 2 * g + k))
        def _():
            pltpu.make_async_remote_copy(
                src_ref=fin.at[0, 0:2],
                dst_ref=landed.at[k],
                send_sem=fsend.at[0],
                recv_sem=frecv.at[k],
                device_id=(s, r),
                device_id_type=MESH,
            ).wait_recv()

    out[...] = landed[...]

    for copy in swap:
        copy.wait_send()
    gathers(False)

    @pl.when((m > 0) & (m < mirror))
    def _():
        forward_a().wait_send()

    @pl.when(m < mirror)
    def _():
        forward_b().wait_send()

    @pl.when(m == stages - 1)
    def _():
        each_piece(lambda copy: copy.wait_send())


def solution(mesh):
    n_seg = mesh.shape["segment"]
    n_row = mesh.shape["row"]
    pieces = n_seg // 2
    cw = 2 * TILE // n_seg
    f32 = jnp.float32
    vmem = pl.BlockSpec(memory_space=pltpu.VMEM)

    def on_device(*args):
        dma = pltpu.SemaphoreType.DMA
        return pl.pallas_call(
            functools.partial(level_kernel, n_seg, n_row),
            out_shape=jax.ShapeDtypeStruct((2, 2, cw, C), f32),
            in_specs=[pl.BlockSpec(memory_space=pl.ANY)] * 8,
            out_specs=vmem,
            scratch_shapes=[
                pltpu.VMEM((2, 2, 2 * TILE, C), f32),
                pltpu.VMEM((1, 3, 3, C, C), f32),
                pltpu.VMEM((1, 3, 3, C, C), f32),
                pltpu.VMEM((2, C, C), f32),
                pltpu.VMEM((4, 1, C), f32),
                pltpu.VMEM((4, 4, C), f32),
                pltpu.VMEM((12, 4, C), f32),
                pltpu.VMEM((12, RING, C), f32),
                pltpu.VMEM((12, RING, C), f32),
                pltpu.VMEM((12, RING, C), f32),
                pltpu.VMEM((12, RING, C), f32),
                pltpu.VMEM((12, RING, C), f32),
                pltpu.VMEM((12, RING, C), f32),
                pltpu.VMEM((4, TILE, C), f32),
                pltpu.VMEM((pieces, 4, cw, C), f32),
                pltpu.VMEM((2, 2, cw, C), f32),
                pltpu.VMEM((1, 3, 3, C, C), f32),
                pltpu.VMEM((1, 3, 3, C, C), f32),
                pltpu.VMEM((4, 1, C), f32),
                pltpu.VMEM((2, 4, 1, C), f32),
                pltpu.VMEM((2, 2, 9 * C, 3 * C), f32),
                pltpu.VMEM((8, RING, C), f32),
                pltpu.VMEM((4, TILE, C), f32),
                pltpu.VMEM((8, RING, C), f32),
                pltpu.VMEM((4, TILE, C), f32),
                pltpu.VMEM((RING, C), f32),
                pltpu.VMEM((RING, C), f32),
                dma((3,)),
                dma((3,)),
                dma((12,)),
                dma((12,)),
                dma((6,)),
                dma((6,)),
                dma((2,)),
                dma((2,)),
                dma((2 * pieces,)),
                dma((2,)),
                dma((8,)),
            ],
            compiler_params=pltpu.CompilerParams(
                collective_id=0, has_side_effects=True, vmem_limit_bytes=60 * 1024 * 1024
            ),
        )(*args)

    return jax.shard_map(
        on_device,
        mesh=mesh,
        in_specs=(
            P(None, "row", None, None),
            P("segment", None, None, None, None),
            P("segment", None, None, None, None),
            P(),
            P("segment", None),
            P("segment", None),
            P("segment", None),
            P("segment", None),
        ),
        out_specs=P(None, "row", "segment", None),
        check_vma=False,
    )
```

```python
import functools

import jax
import jax.numpy as jnp
from jax import lax
from jax.experimental import pallas as pl
from jax.experimental.pallas import tpu as pltpu
from jax.sharding import PartitionSpec as P

MESH = pl.DeviceIdType.MESH
C = 128
TILE = 32
RING = 40
STRIP = 8


def split(x):
    high = x.astype(jnp.bfloat16).astype(jnp.float32)
    return high, x - high


def silu(u):
    return u / (1.0 + jnp.exp(-u))


def level_kernel(
    n_seg,
    n_row,
    img_hbm,
    w1_hbm,
    w2_hbm,
    skipk_hbm,
    g1_hbm,
    b1_hbm,
    g2_hbm,
    b2_hbm,
    out,
    img,
    w1,
    w2,
    skipk,
    ovec,
    sout,
    sin,
    xbuf,
    xh,
    xl,
    hh,
    hl,
    h1,
    yout,
    fin,
    landed,
    pw1,
    pw2,
    pvec,
    vecs,
    wp,
    ska,
    skb,
    ea,
    eb,
    m0,
    m2,
    wsend,
    wrecv,
    gsend,
    grecv,
    msend,
    mrecv,
    ssend,
    srecv,
    fsend,
    frecv,
    lsem,
):
    stages = n_seg // 2
    mirror = stages // 2
    relayed = mirror > 1
    groups = n_row // 2
    pieces = n_seg // 2
    cw = 2 * TILE // n_seg
    s = lax.axis_index("segment")
    r = lax.axis_index("row")
    m = s // 2
    c = s % 2
    g = r // 2
    slab = r % 2
    up = (g > 0).astype(jnp.int32)
    down = (g < groups - 1).astype(jnp.int32)
    valid = 1 + up + down
    inside = {-1: g > 0, 0: g >= 0, 1: g < groups - 1}

    def greet(cond, seg, row):
        @pl.when(cond)
        def _():
            pl.semaphore_signal(barrier, inc=1, device_id=(seg, row), device_id_type=MESH)

    first_skip = jnp.maximum(2 * (m - mirror), 0)
    loads = [
        pltpu.make_async_copy(a, b, lsem.at[i])
        for i, (a, b) in enumerate(
            [
                (img_hbm, img),
                (w1_hbm, w1),
                (w2_hbm, w2),
                (skipk_hbm.at[pl.ds(first_skip, 2)], skipk),
                (g1_hbm, ovec.at[0]),
                (b1_hbm, ovec.at[1]),
                (g2_hbm, ovec.at[2]),
                (b2_hbm, ovec.at[3]),
            ]
        )
    ]
    for copy in loads:
        copy.start()

    xbuf[...] = jnp.zeros_like(xbuf)
    sin[...] = jnp.zeros_like(sin)

    barrier = pltpu.get_barrier_semaphore()
    greet(s >= 0, s + 1 - 2 * c, r)
    for d in (-1, 0, 1):
        greet(inside[d] & (m > 0), s - 2, r + 2 * d)
        greet(inside[d] & (m > 0), s - 1 - 2 * c, r + 2 * d)
        for q in (0, 1):
            other = 2 * (g + d) + q
            greet(inside[d] & (m == 0) & (other != r), s, other)
    greet(m > mirror, 2 * (stages - m) + c, r)
    if relayed:
        greet((m >= mirror) & (m < stages - 1), 2 * (stages - 1 - m) + c, r)
        greet(m == stages - 1, 2 + c, r)
        greet(m == 1, c, r)
    else:
        greet(m >= mirror, 2 * (stages - 1 - m) + c, r)
    source = n_seg - 2 + s // pieces
    for k in (0, 1):
        greet((s != source) | (r != 2 * g + k), source, 2 * g + k)

    one = jnp.int32(1)
    zero = jnp.int32(0)
    expected = (
        1
        + jnp.where(m < stages - 1, 2 * valid, zero)
        + jnp.where(m == 0, 2 * valid - 1, zero)
        + jnp.where((m > 0) & (m < mirror), one, zero)
        + jnp.where(m < mirror, one, zero)
        + (jnp.where(m == 1, one, zero) if relayed else zero)
        + jnp.where(m == stages - 1, 2 * pieces - c, zero)
    )
    pl.semaphore_wait(barrier, expected)

    def swaps():
        pairs = [(w1, pw1), (w2, pw2), (ovec, pvec)]
        return [
            pltpu.make_async_remote_copy(
                src_ref=a,
                dst_ref=b,
                send_sem=wsend.at[i],
                recv_sem=wrecv.at[i],
                device_id=(s + 1 - 2 * c, r),
                device_id_type=MESH,
            )
            for i, (a, b) in enumerate(pairs)
        ]

    swap = swaps()

    own = pl.ds(pl.multiple_of(TILE * c, TILE), TILE)
    strip = pl.ds(pl.multiple_of(TILE - STRIP * c, STRIP), STRIP)

    def gathers(start):
        for d in (-1, 1, 0):
            for q in (0, 1):
                other = 2 * (g + d) + q
                offset = 2 * slab - 4 * d + 4
                index = (2 * (1 - d) + slab) * 2

                @pl.when((m == 0) & inside[d] & (other != r))
                def _():
                    for kind, (a, b) in enumerate(
                        (
                            (img.at[q, :, own, :], (0, TILE)),
                            (img.at[q, :, strip, :], (TILE, STRIP)),
                        )
                    ):
                        copy = pltpu.make_async_remote_copy(
                            src_ref=a,
                            dst_ref=xbuf.at[pl.ds(offset, 2), b[0] : b[0] + b[1], :],
                            send_sem=gsend.at[((d + 1) * 2 + q) * 2 + kind],
                            recv_sem=grecv.at[index + kind],
                            device_id=(s, other),
                            device_id_type=MESH,
                        )
                        if start:
                            copy.start()
                        else:
                            copy.wait_send()

    loads[0].wait()
    gathers(True)

    for copy in loads[1:]:
        copy.wait()
    for copy in swap:
        copy.start()

    column = lax.broadcasted_iota(jnp.int32, (RING, C), 0)
    m0[...] = jnp.where((column == 0) & (c == 0), 0.0, 1.0)
    m2[...] = jnp.where((column == TILE - 1) & (c == 1), 0.0, 1.0)

    def prepare(slot, conv, ref):
        for a in range(3):
            for b in range(3):
                high, low = split(ref[0, a, b])
                cols = pl.ds(b * C, C)
                wp[slot, conv, pl.ds(a * C, C), cols] = high
                wp[slot, conv, pl.ds((3 + a) * C, C), cols] = high
                wp[slot, conv, pl.ds((6 + a) * C, C), cols] = low

    prepare(c, 0, w1)
    prepare(c, 1, w2)
    vecs[c] = ovec[...]
    swap[0].wait_recv()
    prepare(1 - c, 0, pw1)
    swap[1].wait_recv()
    prepare(1 - c, 1, pw2)
    swap[2].wait_recv()
    vecs[1 - c] = pvec[...]

    def skip_term(src, dst, which):
        rows, columns = src.shape[:2]
        xv, xw = split(src[...].reshape(rows * columns, C))
        kh, kl = split(skipk[which])
        dot = functools.partial(jnp.dot, preferred_element_type=jnp.float32)
        term = dot(xv, kh) + (dot(xv, kl) + dot(xw, kh))
        dst[...] = term.reshape(rows, columns, C)

    ea[...] = jnp.zeros_like(ea)
    eb[...] = jnp.zeros_like(eb)

    def forward_a():
        return pltpu.make_async_remote_copy(
            src_ref=xbuf.at[2:10],
            dst_ref=ska,
            send_sem=ssend.at[0],
            recv_sem=srecv.at[0],
            device_id=(2 * (stages - m) + c, r),
            device_id_type=MESH,
        )

    def forward_b():
        return pltpu.make_async_remote_copy(
            src_ref=h1.at[4:8, 0:TILE],
            dst_ref=skb,
            send_sem=ssend.at[1],
            recv_sem=srecv.at[1],
            device_id=(
                jnp.where(m == 0, 2, 2 * (stages - 1 - m)) + c if relayed else s + 2,
                r,
            ),
            device_id_type=MESH,
        )

    def relay():
        return pltpu.make_async_remote_copy(
            src_ref=skb,
            dst_ref=skb,
            send_sem=ssend.at[2],
            recv_sem=srecv.at[1],
            device_id=(2 * (stages - 1) + c, r),
            device_id_type=MESH,
        )

    @pl.when(m > mirror)
    def _():
        forward_a().wait_recv()
        skip_term(ska, ea, 0)

    @pl.when(m >= mirror)
    def _():
        forward_b().wait_recv()
        skip_term(skb, eb, 1)

    def handover(d, kind):
        slot = 1 - d
        if kind == 0:
            src = yout
            dst = xbuf.at[4 * slot : 4 * slot + 4, 0:TILE, :]
            seg = s + 2
        else:
            src = sout
            dst = sin.at[4 * slot : 4 * slot + 4]
            seg = s + 3 - 2 * c
        return pltpu.make_async_remote_copy(
            src_ref=src,
            dst_ref=dst,
            send_sem=msend.at[2 * (d + 1) + kind],
            recv_sem=mrecv.at[2 * slot + kind],
            device_id=(seg, r + 2 * d),
            device_id_type=MESH,
        )

    for d in (-1, 0, 1):

        @pl.when((m == 0) & inside[d])
        def _():
            for p in (0, 1):
                index = (2 * (1 + d) + p) * 2

                @pl.when((2 * (g + d) + p) != r)
                def _():
                    for kind, b in enumerate(((0, TILE), (TILE, STRIP))):
                        rows = 2 * p + 4 * d + 4
                        pltpu.make_async_remote_copy(
                            src_ref=xbuf.at[rows : rows + 2, b[0] : b[0] + b[1], :],
                            dst_ref=xbuf.at[rows : rows + 2, b[0] : b[0] + b[1], :],
                            send_sem=gsend.at[0],
                            recv_sem=grecv.at[index + kind],
                            device_id=(s, r),
                            device_id_type=MESH,
                        ).wait_recv()

        @pl.when((m > 0) & inside[d])
        def _():
            for kind in (0, 1):
                handover(-d, kind).wait_recv()

    for q in (0, 1):

        @pl.when((m == 0) & (slab == q))
        def _():
            xbuf[4 + 2 * q : 6 + 2 * q, 0:TILE, :] = img[q, :, own, :]
            xbuf[4 + 2 * q : 6 + 2 * q, TILE:RING, :] = img[q, :, strip, :]

    @pl.when(m > 0)
    def _():
        xbuf[:, TILE : TILE + 4] = sin[...]
        xbuf[:, TILE + 4 : RING] = sin[...]

    @pl.when(m == mirror)
    def _():
        skip_term(xbuf.at[2:10], ea, 0)

    def conv(high, low, first, rows, slot, which):
        def part(ref, a):
            return ref[first - 1 + a : first - 1 + a + rows].reshape(rows * RING, C)

        hs = [part(high, a) for a in range(3)]
        ls = [part(low, a) for a in range(3)]
        left = jnp.concatenate(hs + ls + hs, axis=1)
        acc = jnp.dot(left, wp[slot, which], preferred_element_type=jnp.float32)
        left_tap, middle, right_tap = [
            acc[:, b * C : (b + 1) * C].reshape(rows, RING, C) for b in range(3)
        ]
        return (
            pltpu.roll(left_tap, 1, 1) * m0[...][None]
            + middle
            + pltpu.roll(right_tap, RING - 1, 1) * m2[...][None]
        )

    def inside_rows(value, first):
        row = 4 * g - 4 + first + lax.broadcasted_iota(jnp.int32, value.shape, 0)
        return jnp.where((row >= 0) & (row < 4 * groups), value, 0.0)

    def vec(slot, i):
        return vecs[slot, i].reshape(1, 1, C)

    def store_split(high, low, first, value):
        top, rest = split(value)
        high[first : first + value.shape[0]] = top
        low[first : first + value.shape[0]] = rest

    store_split(xh, xl, 0, xbuf[...])
    hidden = inside_rows(silu(vec(0, 0) * conv(xh, xl, 1, 10, 0, 0) + vec(0, 1)), 1)
    store_split(hh, hl, 1, hidden)
    value = xbuf[2:10] + silu(vec(0, 2) * (conv(hh, hl, 2, 8, 0, 1) + ea[...]) + vec(0, 3))
    value = inside_rows(value, 2)
    h1[2:10] = value
    store_split(xh, xl, 2, value)

    @pl.when(m == mirror - 1)
    def _():
        forward_b().start()

    hidden = inside_rows(silu(vec(1, 0) * conv(xh, xl, 3, 6, 1, 0) + vec(1, 1)), 3)
    store_split(hh, hl, 3, hidden)
    second = conv(hh, hl, 4, 4, 1, 1)[:, 0:TILE] + eb[...]
    value = h1[4:8, 0:TILE] + silu(vec(1, 2) * second + vec(1, 3))

    def handovers(action):
        for d, kind in ((-1, 1), (1, 1), (-1, 0), (1, 0), (0, 1), (0, 0)):

            @pl.when(inside[d])
            def _():
                action(handover(d, kind))

    @pl.when(m < stages - 1)
    def _():
        yout[...] = value
        sout[...] = jnp.where(c == 0, value[:, TILE - 4 :], value[:, :4])
        handovers(lambda copy: copy.start())
        handovers(lambda copy: copy.wait_send())

    @pl.when((m > 0) & (m < mirror))
    def _():
        forward_a().start()

    @pl.when(m < mirror - 1)
    def _():
        forward_b().start()

    if relayed:

        @pl.when(m == 1)
        def _():
            forward_b().wait_recv()
            relay().start()
            relay().wait_send()

    def scatter(i, p):
        return pltpu.make_async_remote_copy(
            src_ref=fin.at[i, 2 * p : 2 * p + 2],
            dst_ref=landed.at[slab],
            send_sem=fsend.at[2 * i + p],
            recv_sem=frecv.at[slab],
            device_id=(pieces * c + i, 2 * g + p),
            device_id_type=MESH,
        )

    def each_piece(action):
        for i in range(pieces):
            for p in (0, 1):

                @pl.when((pieces * c + i != s) | (2 * g + p != r))
                def _():
                    action(scatter(i, p))

    @pl.when(m == stages - 1)
    def _():
        for i in range(pieces):
            fin[i] = value[:, i * cw : (i + 1) * cw, :]
        each_piece(lambda copy: copy.start())

        for p in (0, 1):

            @pl.when((c == 1) & (slab == p))
            def _():
                landed[p] = fin[pieces - 1, 2 * p : 2 * p + 2]

    for k in (0, 1):

        @pl.when((s != source) | (r != 2 * g + k))
        def _():
            pltpu.make_async_remote_copy(
                src_ref=fin.at[0, 0:2],
                dst_ref=landed.at[k],
                send_sem=fsend.at[0],
                recv_sem=frecv.at[k],
                device_id=(s, r),
                device_id_type=MESH,
            ).wait_recv()

    out[...] = landed[...]

    for copy in swap:
        copy.wait_send()
    gathers(False)

    @pl.when((m > 0) & (m < mirror))
    def _():
        forward_a().wait_send()

    @pl.when(m < mirror)
    def _():
        forward_b().wait_send()

    @pl.when(m == stages - 1)
    def _():
        each_piece(lambda copy: copy.wait_send())


def solution(mesh):
    n_seg = mesh.shape["segment"]
    n_row = mesh.shape["row"]
    pieces = n_seg // 2
    cw = 2 * TILE // n_seg
    f32 = jnp.float32
    vmem = pl.BlockSpec(memory_space=pltpu.VMEM)

    def on_device(*args):
        dma = pltpu.SemaphoreType.DMA
        return pl.pallas_call(
            functools.partial(level_kernel, n_seg, n_row),
            out_shape=jax.ShapeDtypeStruct((2, 2, cw, C), f32),
            in_specs=[pl.BlockSpec(memory_space=pl.ANY)] * 8,
            out_specs=vmem,
            scratch_shapes=[
                pltpu.VMEM((2, 2, 2 * TILE, C), f32),
                pltpu.VMEM((1, 3, 3, C, C), f32),
                pltpu.VMEM((1, 3, 3, C, C), f32),
                pltpu.VMEM((2, C, C), f32),
                pltpu.VMEM((4, 1, C), f32),
                pltpu.VMEM((4, 4, C), f32),
                pltpu.VMEM((12, 4, C), f32),
                pltpu.VMEM((12, RING, C), f32),
                pltpu.VMEM((12, RING, C), f32),
                pltpu.VMEM((12, RING, C), f32),
                pltpu.VMEM((12, RING, C), f32),
                pltpu.VMEM((12, RING, C), f32),
                pltpu.VMEM((12, RING, C), f32),
                pltpu.VMEM((4, TILE, C), f32),
                pltpu.VMEM((pieces, 4, cw, C), f32),
                pltpu.VMEM((2, 2, cw, C), f32),
                pltpu.VMEM((1, 3, 3, C, C), f32),
                pltpu.VMEM((1, 3, 3, C, C), f32),
                pltpu.VMEM((4, 1, C), f32),
                pltpu.VMEM((2, 4, 1, C), f32),
                pltpu.VMEM((2, 2, 9 * C, 3 * C), f32),
                pltpu.VMEM((8, RING, C), f32),
                pltpu.VMEM((4, TILE, C), f32),
                pltpu.VMEM((8, RING, C), f32),
                pltpu.VMEM((4, TILE, C), f32),
                pltpu.VMEM((RING, C), f32),
                pltpu.VMEM((RING, C), f32),
                dma((3,)),
                dma((3,)),
                dma((12,)),
                dma((12,)),
                dma((6,)),
                dma((6,)),
                dma((3,)),
                dma((2,)),
                dma((2 * pieces,)),
                dma((2,)),
                dma((8,)),
            ],
            compiler_params=pltpu.CompilerParams(
                collective_id=0, has_side_effects=True, vmem_limit_bytes=60 * 1024 * 1024
            ),
        )(*args)

    return jax.shard_map(
        on_device,
        mesh=mesh,
        in_specs=(
            P(None, "row", None, None),
            P("segment", None, None, None, None),
            P("segment", None, None, None, None),
            P(),
            P("segment", None),
            P("segment", None),
            P("segment", None),
            P("segment", None),
        ),
        out_specs=P(None, "row", "segment", None),
        check_vma=False,
    )
```

```python
import functools

import jax
import jax.numpy as jnp
from jax import lax
from jax.experimental import pallas as pl
from jax.experimental.pallas import tpu as pltpu
from jax.sharding import PartitionSpec as P

MESH = pl.DeviceIdType.MESH
C = 128
TILE = 32
RING = 40
STRIP = 8


def split(x):
    high = x.astype(jnp.bfloat16).astype(jnp.float32)
    return high, x - high


def silu(u):
    return u * (0.5 + 0.5 * jnp.tanh(0.5 * u))


def level_kernel(
    n_seg,
    n_row,
    img_hbm,
    w1_hbm,
    w2_hbm,
    skipk_hbm,
    g1_hbm,
    b1_hbm,
    g2_hbm,
    b2_hbm,
    out,
    img,
    w1,
    w2,
    skipk,
    ovec,
    sout,
    sin,
    xbuf,
    xh,
    xl,
    hh,
    hl,
    h1,
    yout,
    fin,
    landed,
    pw1,
    pw2,
    pvec,
    vecs,
    wp,
    ska,
    skb,
    ea,
    eb,
    m0,
    m2,
    wsend,
    wrecv,
    gsend,
    grecv,
    msend,
    mrecv,
    ssend,
    srecv,
    fsend,
    frecv,
    lsem,
):
    stages = n_seg // 2
    mirror = stages // 2
    relayed = mirror > 1
    groups = n_row // 2
    pieces = n_seg // 2
    cw = 2 * TILE // n_seg
    s = lax.axis_index("segment")
    r = lax.axis_index("row")
    m = s // 2
    c = s % 2
    g = r // 2
    slab = r % 2
    up = (g > 0).astype(jnp.int32)
    down = (g < groups - 1).astype(jnp.int32)
    valid = 1 + up + down
    inside = {-1: g > 0, 0: g >= 0, 1: g < groups - 1}
    long_way = 2 * (g % 2) - 1

    def within(d):
        return (g + d >= 0) & (g + d < groups)


    def greet(cond, seg, row):
        @pl.when(cond)
        def _():
            pl.semaphore_signal(barrier, inc=1, device_id=(seg, row), device_id_type=MESH)

    first_skip = jnp.maximum(2 * (m - mirror), 0)
    loads = [
        pltpu.make_async_copy(a, b, lsem.at[i])
        for i, (a, b) in enumerate(
            [
                (img_hbm, img),
                (w1_hbm, w1),
                (w2_hbm, w2),
                (skipk_hbm.at[pl.ds(first_skip, 2)], skipk),
                (g1_hbm, ovec.at[0]),
                (b1_hbm, ovec.at[1]),
                (g2_hbm, ovec.at[2]),
                (b2_hbm, ovec.at[3]),
            ]
        )
    ]
    for copy in loads:
        copy.start()

    xbuf[...] = jnp.zeros_like(xbuf)
    sin[...] = jnp.zeros_like(sin)

    barrier = pltpu.get_barrier_semaphore()
    greet(s >= 0, s + 1 - 2 * c, r)
    for d in (-1, 0, 1):
        greet(inside[d] & (m > 0), s - 2, r + 2 * d)
        greet(inside[d] & (m > 0), s - 1 - 2 * c, r + 2 * d)
        for q in (0, 1):
            other = 2 * (g + d) + q
            greet(inside[d] & (m == 0) & (other != r), s, other)
    greet(m > mirror, 2 * (stages - m) + c, r)
    if relayed:
        greet((m >= mirror) & (m < stages - 1), 2 * (stages - 1 - m) + c, r)
        greet(m == stages - 1, 2 + c, r)
        greet(m == 1, c, r)
    else:
        greet(m >= mirror, 2 * (stages - 1 - m) + c, r)
    source = n_seg - 2 + s // pieces
    for k in (0, 1):
        greet((s != source) | (r != 2 * g + k), source, 2 * g + k)

    one = jnp.int32(1)
    zero = jnp.int32(0)
    expected = (
        1
        + jnp.where(m < stages - 1, 2 * valid, zero)
        + jnp.where(m == 0, 2 * valid - 1, zero)
        + jnp.where((m > 0) & (m < mirror), one, zero)
        + jnp.where(m < mirror, one, zero)
        + (jnp.where(m == 1, one, zero) if relayed else zero)
        + jnp.where(m == stages - 1, 2 * pieces - c, zero)
    )
    pl.semaphore_wait(barrier, expected)

    def swaps():
        pairs = [(w1, pw1), (w2, pw2), (ovec, pvec)]
        return [
            pltpu.make_async_remote_copy(
                src_ref=a,
                dst_ref=b,
                send_sem=wsend.at[i],
                recv_sem=wrecv.at[i],
                device_id=(s + 1 - 2 * c, r),
                device_id_type=MESH,
            )
            for i, (a, b) in enumerate(pairs)
        ]

    swap = swaps()

    own = pl.ds(pl.multiple_of(TILE * c, TILE), TILE)
    strip = pl.ds(pl.multiple_of(TILE - STRIP * c, STRIP), STRIP)

    def gathers(start):
        for d in (long_way, -long_way, 0):
            for q in (0, 1):
                other = 2 * (g + d) + q
                offset = 2 * slab - 4 * d + 4
                index = (2 * (1 - d) + slab) * 2

                @pl.when((m == 0) & within(d) & (other != r))
                def _():
                    for kind, (a, b) in enumerate(
                        (
                            (img.at[q, :, own, :], (0, TILE)),
                            (img.at[q, :, strip, :], (TILE, STRIP)),
                        )
                    ):
                        copy = pltpu.make_async_remote_copy(
                            src_ref=a,
                            dst_ref=xbuf.at[pl.ds(offset, 2), b[0] : b[0] + b[1], :],
                            send_sem=gsend.at[((d + 1) * 2 + q) * 2 + kind],
                            recv_sem=grecv.at[index + kind],
                            device_id=(s, other),
                            device_id_type=MESH,
                        )
                        if start:
                            copy.start()
                        else:
                            copy.wait_send()

    loads[0].wait()
    gathers(True)

    for copy in loads[1:]:
        copy.wait()
    for copy in swap:
        copy.start()

    column = lax.broadcasted_iota(jnp.int32, (RING, C), 0)
    m0[...] = jnp.where((column == 0) & (c == 0), 0.0, 1.0)
    m2[...] = jnp.where((column == TILE - 1) & (c == 1), 0.0, 1.0)

    def prepare(slot, conv, ref):
        for a in range(3):
            for b in range(3):
                high, low = split(ref[0, a, b])
                cols = pl.ds(b * C, C)
                wp[slot, conv, pl.ds(a * C, C), cols] = high
                wp[slot, conv, pl.ds((3 + a) * C, C), cols] = high
                wp[slot, conv, pl.ds((6 + a) * C, C), cols] = low

    prepare(c, 0, w1)
    prepare(c, 1, w2)
    vecs[c] = ovec[...]
    swap[0].wait_recv()
    prepare(1 - c, 0, pw1)
    swap[1].wait_recv()
    prepare(1 - c, 1, pw2)
    swap[2].wait_recv()
    vecs[1 - c] = pvec[...]

    def skip_term(src, dst, which):
        rows, columns = src.shape[:2]
        xv, xw = split(src[...].reshape(rows * columns, C))
        kh, kl = split(skipk[which])
        dot = functools.partial(jnp.dot, preferred_element_type=jnp.float32)
        term = dot(xv, kh) + (dot(xv, kl) + dot(xw, kh))
        dst[...] = term.reshape(rows, columns, C)

    ea[...] = jnp.zeros_like(ea)
    eb[...] = jnp.zeros_like(eb)

    def forward_a():
        return pltpu.make_async_remote_copy(
            src_ref=xbuf.at[2:10],
            dst_ref=ska,
            send_sem=ssend.at[0],
            recv_sem=srecv.at[0],
            device_id=(2 * (stages - m) + c, r),
            device_id_type=MESH,
        )

    def forward_b():
        return pltpu.make_async_remote_copy(
            src_ref=h1.at[4:8, 0:TILE],
            dst_ref=skb,
            send_sem=ssend.at[1],
            recv_sem=srecv.at[1],
            device_id=(
                jnp.where(m == 0, 2, 2 * (stages - 1 - m)) + c if relayed else s + 2,
                r,
            ),
            device_id_type=MESH,
        )

    def relay():
        return pltpu.make_async_remote_copy(
            src_ref=skb,
            dst_ref=skb,
            send_sem=ssend.at[2],
            recv_sem=srecv.at[1],
            device_id=(2 * (stages - 1) + c, r),
            device_id_type=MESH,
        )

    @pl.when(m > mirror)
    def _():
        forward_a().wait_recv()
        skip_term(ska, ea, 0)

    @pl.when(m >= mirror)
    def _():
        forward_b().wait_recv()
        skip_term(skb, eb, 1)

    def handover(d, kind):
        slot = 1 - d
        if kind == 0:
            src = yout
            dst = xbuf.at[pl.ds(4 * slot, 4), 0:TILE, :]
            seg = s + 2
        else:
            src = sout
            dst = sin.at[pl.ds(4 * slot, 4)]
            seg = s + 3 - 2 * c
        return pltpu.make_async_remote_copy(
            src_ref=src,
            dst_ref=dst,
            send_sem=msend.at[2 * (d + 1) + kind],
            recv_sem=mrecv.at[2 * slot + kind],
            device_id=(seg, r + 2 * d),
            device_id_type=MESH,
        )

    for d in (-1, 0, 1):

        @pl.when((m == 0) & inside[d])
        def _():
            for p in (0, 1):
                index = (2 * (1 + d) + p) * 2

                @pl.when((2 * (g + d) + p) != r)
                def _():
                    for kind, b in enumerate(((0, TILE), (TILE, STRIP))):
                        rows = 2 * p + 4 * d + 4
                        pltpu.make_async_remote_copy(
                            src_ref=xbuf.at[rows : rows + 2, b[0] : b[0] + b[1], :],
                            dst_ref=xbuf.at[rows : rows + 2, b[0] : b[0] + b[1], :],
                            send_sem=gsend.at[0],
                            recv_sem=grecv.at[index + kind],
                            device_id=(s, r),
                            device_id_type=MESH,
                        ).wait_recv()

        @pl.when((m > 0) & inside[d])
        def _():
            for kind in (0, 1):
                handover(-d, kind).wait_recv()

    for q in (0, 1):

        @pl.when((m == 0) & (slab == q))
        def _():
            xbuf[4 + 2 * q : 6 + 2 * q, 0:TILE, :] = img[q, :, own, :]
            xbuf[4 + 2 * q : 6 + 2 * q, TILE:RING, :] = img[q, :, strip, :]

    @pl.when(m > 0)
    def _():
        xbuf[:, TILE : TILE + 4] = sin[...]
        xbuf[:, TILE + 4 : RING] = sin[...]

    @pl.when(m == mirror)
    def _():
        skip_term(xbuf.at[2:10], ea, 0)

    def conv(high, low, first, rows, slot, which):
        def part(ref, a):
            return ref[first - 1 + a : first - 1 + a + rows].reshape(rows * RING, C)

        hs = [part(high, a) for a in range(3)]
        ls = [part(low, a) for a in range(3)]
        left = jnp.concatenate(hs + ls + hs, axis=1)
        acc = jnp.dot(left, wp[slot, which], preferred_element_type=jnp.float32)
        left_tap, middle, right_tap = [
            acc[:, b * C : (b + 1) * C].reshape(rows, RING, C) for b in range(3)
        ]
        return (
            pltpu.roll(left_tap, 1, 1) * m0[...][None]
            + middle
            + pltpu.roll(right_tap, RING - 1, 1) * m2[...][None]
        )

    def inside_rows(value, first):
        row = 4 * g - 4 + first + lax.broadcasted_iota(jnp.int32, value.shape, 0)
        return jnp.where((row >= 0) & (row < 4 * groups), value, 0.0)

    def vec(slot, i):
        return vecs[slot, i].reshape(1, 1, C)

    def store_split(high, low, first, value):
        top, rest = split(value)
        high[first : first + value.shape[0]] = top
        low[first : first + value.shape[0]] = rest

    store_split(xh, xl, 0, xbuf[...])
    hidden = inside_rows(silu(vec(0, 0) * conv(xh, xl, 1, 10, 0, 0) + vec(0, 1)), 1)
    store_split(hh, hl, 1, hidden)
    value = xbuf[2:10] + silu(vec(0, 2) * (conv(hh, hl, 2, 8, 0, 1) + ea[...]) + vec(0, 3))
    value = inside_rows(value, 2)
    h1[2:10] = value
    store_split(xh, xl, 2, value)

    @pl.when(m == mirror - 1)
    def _():
        forward_b().start()

    hidden = inside_rows(silu(vec(1, 0) * conv(xh, xl, 3, 6, 1, 0) + vec(1, 1)), 3)
    store_split(hh, hl, 3, hidden)
    second = conv(hh, hl, 4, 4, 1, 1)[:, 0:TILE] + eb[...]
    value = h1[4:8, 0:TILE] + silu(vec(1, 2) * second + vec(1, 3))

    def handovers(action):
        far = [(d, kind) for kind in (1, 0) for d in (long_way, -long_way)]
        for d, kind in far + [(0, 1), (0, 0)]:

            @pl.when(within(d))
            def _():
                action(handover(d, kind))

    @pl.when(m < stages - 1)
    def _():
        yout[...] = value
        sout[...] = jnp.where(c == 0, value[:, TILE - 4 :], value[:, :4])
        handovers(lambda copy: copy.start())
        handovers(lambda copy: copy.wait_send())

    @pl.when((m > 0) & (m < mirror))
    def _():
        forward_a().start()

    @pl.when(m < mirror - 1)
    def _():
        forward_b().start()

    if relayed:

        @pl.when(m == 1)
        def _():
            forward_b().wait_recv()
            relay().start()
            relay().wait_send()

    def scatter(i, p):
        return pltpu.make_async_remote_copy(
            src_ref=fin.at[i, 2 * p : 2 * p + 2],
            dst_ref=landed.at[slab],
            send_sem=fsend.at[2 * i + p],
            recv_sem=frecv.at[slab],
            device_id=(pieces * c + i, 2 * g + p),
            device_id_type=MESH,
        )

    def each_piece(action):
        for i in range(pieces):
            for p in (0, 1):

                @pl.when((pieces * c + i != s) | (2 * g + p != r))
                def _():
                    action(scatter(i, p))

    @pl.when(m == stages - 1)
    def _():
        for i in range(pieces):
            fin[i] = value[:, i * cw : (i + 1) * cw, :]
        each_piece(lambda copy: copy.start())

        for p in (0, 1):

            @pl.when((c == 1) & (slab == p))
            def _():
                landed[p] = fin[pieces - 1, 2 * p : 2 * p + 2]

    for k in (0, 1):

        @pl.when((s != source) | (r != 2 * g + k))
        def _():
            pltpu.make_async_remote_copy(
                src_ref=fin.at[0, 0:2],
                dst_ref=landed.at[k],
                send_sem=fsend.at[0],
                recv_sem=frecv.at[k],
                device_id=(s, r),
                device_id_type=MESH,
            ).wait_recv()

    out[...] = landed[...]

    for copy in swap:
        copy.wait_send()
    gathers(False)

    @pl.when((m > 0) & (m < mirror))
    def _():
        forward_a().wait_send()

    @pl.when(m < mirror)
    def _():
        forward_b().wait_send()

    @pl.when(m == stages - 1)
    def _():
        each_piece(lambda copy: copy.wait_send())


def solution(mesh):
    n_seg = mesh.shape["segment"]
    n_row = mesh.shape["row"]
    pieces = n_seg // 2
    cw = 2 * TILE // n_seg
    f32 = jnp.float32
    vmem = pl.BlockSpec(memory_space=pltpu.VMEM)

    def on_device(*args):
        dma = pltpu.SemaphoreType.DMA
        return pl.pallas_call(
            functools.partial(level_kernel, n_seg, n_row),
            out_shape=jax.ShapeDtypeStruct((2, 2, cw, C), f32),
            in_specs=[pl.BlockSpec(memory_space=pl.ANY)] * 8,
            out_specs=vmem,
            scratch_shapes=[
                pltpu.VMEM((2, 2, 2 * TILE, C), f32),
                pltpu.VMEM((1, 3, 3, C, C), f32),
                pltpu.VMEM((1, 3, 3, C, C), f32),
                pltpu.VMEM((2, C, C), f32),
                pltpu.VMEM((4, 1, C), f32),
                pltpu.VMEM((4, 4, C), f32),
                pltpu.VMEM((12, 4, C), f32),
                pltpu.VMEM((12, RING, C), f32),
                pltpu.VMEM((12, RING, C), f32),
                pltpu.VMEM((12, RING, C), f32),
                pltpu.VMEM((12, RING, C), f32),
                pltpu.VMEM((12, RING, C), f32),
                pltpu.VMEM((12, RING, C), f32),
                pltpu.VMEM((4, TILE, C), f32),
                pltpu.VMEM((pieces, 4, cw, C), f32),
                pltpu.VMEM((2, 2, cw, C), f32),
                pltpu.VMEM((1, 3, 3, C, C), f32),
                pltpu.VMEM((1, 3, 3, C, C), f32),
                pltpu.VMEM((4, 1, C), f32),
                pltpu.VMEM((2, 4, 1, C), f32),
                pltpu.VMEM((2, 2, 9 * C, 3 * C), f32),
                pltpu.VMEM((8, RING, C), f32),
                pltpu.VMEM((4, TILE, C), f32),
                pltpu.VMEM((8, RING, C), f32),
                pltpu.VMEM((4, TILE, C), f32),
                pltpu.VMEM((RING, C), f32),
                pltpu.VMEM((RING, C), f32),
                dma((3,)),
                dma((3,)),
                dma((12,)),
                dma((12,)),
                dma((6,)),
                dma((6,)),
                dma((3,)),
                dma((2,)),
                dma((2 * pieces,)),
                dma((2,)),
                dma((8,)),
            ],
            compiler_params=pltpu.CompilerParams(
                collective_id=0, has_side_effects=True, vmem_limit_bytes=60 * 1024 * 1024
            ),
        )(*args)

    return jax.shard_map(
        on_device,
        mesh=mesh,
        in_specs=(
            P(None, "row", None, None),
            P("segment", None, None, None, None),
            P("segment", None, None, None, None),
            P(),
            P("segment", None),
            P("segment", None),
            P("segment", None),
            P("segment", None),
        ),
        out_specs=P(None, "row", "segment", None),
        check_vma=False,
    )
```
